32 devices in a mesh: gx: 4 (over y, x), gy: 2 (over core), gz: 4 (over z).
Axes of the slice: x: 2, y: 2, z: 4, core: 2. Of those that a mesh axis runs over, the one named last changes fastest.
Arguments:
- right_side: float32 [64, 128, 1024], P('gx', 'gy', 'gz'), may hold values from -8 to 8
- cell_type: int32 [64, 128, 1024], P('gx', 'gy', 'gz'), may hold values from 0 to 2
- relax_weight: float32 [64, 128, 1024], P('gx', 'gy', 'gz'), may hold values from 0.25 to 2
Outputs:
- pressure: float32 [64, 128, 1024], P('gx', 'gy', 'gz')
- residual: float32 [64, 128, 1024], P('gx', 'gy', 'gz')
The draws below stay inside these ranges and needn't reach their ends.
Inputs may be any that keep to these rules, and one draw needn't show every extreme that they name: `cell_type`: 0 marks a solid cell, 1 a fluid cell, 2 an empty (air) cell.
All inputs are finite; a program needn't handle non-finite values.
Results may differ from the reference program's by a relative error of at most 0.033.
Values sent between devices are 32-bit elements.
A program may use at most 64 MiB of HBM per device.

```python
import math
import jax
import jax.numpy as jnp

CX = 16
CY = 64
CZ = 256
ITERS = 8
NX = 64
NY = 128
NZ = 1024
N_GX = 4
N_GY = 2
N_GZ = 4


def plant(values, key, low, top_value):
    longest = values.shape.index(max(values.shape))
    spots = []
    for shift in (0, 1):
        where = [jax.random.randint(jax.random.fold_in(key, axis), (), 0, length) for axis, length in enumerate(values.shape)]
        where[longest] = (where[longest] + shift) % values.shape[longest]
        spots.append(tuple(where))
    return values.at[spots[0]].set(low).at[spots[1]].set(top_value)


def level_of(rng, dims, split, smallest, largest):
    factor_of = 1.0
    for dim, shards_of in split:
        heights = jax.random.uniform(jax.random.fold_in(jax.random.fold_in(rng, 6), dim), (shards_of,), jnp.float32, smallest / len(split), largest / len(split))
        factor_of = factor_of * jnp.repeat(jnp.exp(heights), dims[dim] // shards_of).reshape((-1,) + (1,) * (len(dims) - 1 - dim))
    return factor_of


def bell_draw(stream_key, shape, spread, most, pieces=(), kind=jnp.bfloat16):
    result = spread * jax.random.normal(stream_key, shape, jnp.float32)
    if pieces:
        result = result * level_of(stream_key, shape, pieces, -0.22, 0.18)
    return jnp.clip(result, -most, most).astype(kind)


def setup_inputs(seed: int = 0) -> dict:
    splits = jax.random.split(jax.random.key(seed), 4)
    right_side = bell_draw(splits[0], (NX, NY, NZ), 1.0, 8.0, ((0, 4), (1, 2), (2, 4)), jnp.float32)
    cell_type = plant(jax.random.randint(splits[1], (NX, NY, NZ), 0, 3), jax.random.fold_in(splits[1], 1), 0, 2).astype(jnp.int32)
    relax_weight = jnp.clip(jnp.exp(math.log(2.0) - 2.0794415 * jax.random.uniform(splits[2], (NX, NY, NZ), jnp.float32) ** level_of(splits[2], (NX, NY, NZ), ((0, 4), (1, 2), (2, 4)), -0.2, 0.2)), 0.25, 2.0)
    return dict(right_side=right_side, cell_type=cell_type, relax_weight=relax_weight)


def beside(padded):
    total = padded[2:, 1:-1, 1:-1] + padded[:-2, 1:-1, 1:-1]
    total = total + padded[1:-1, 2:, 1:-1] + padded[1:-1, :-2, 1:-1]
    total = total + padded[1:-1, 1:-1, 2:] + padded[1:-1, 1:-1, :-2]
    return total


def split_limbs(product):
    top = jnp.floor(product * (1.0 / 4096.0))
    rest = product - top * 4096.0
    mid = jnp.floor(rest)
    rest = (rest - mid) * 4096.0
    low = jnp.floor(rest)
    rest = (rest - low) * 4096.0
    least = jnp.floor(rest)
    return [least.astype(jnp.int32), low.astype(jnp.int32), mid.astype(jnp.int32), top.astype(jnp.int32)]


def normalize(sums):
    carry = jnp.zeros_like(sums[0])
    limbs_out = []
    for value in sums:
        value = value + carry
        carry = jnp.floor_divide(value, 4096)
        limbs_out.append(value - carry * 4096)
    limbs_out.append(carry)
    return jnp.stack(limbs_out, -1)


def combine(limb_vec):
    parts = limb_vec.astype(jnp.float32)
    total = parts[..., 4] * 16777216.0 + parts[..., 3] * 4096.0
    total = total + parts[..., 2]
    total = total + parts[..., 1] * (1.0 / 4096.0)
    total = total + parts[..., 0] * (1.0 / 16777216.0)
    return total


def dot_field(first, second):
    limbs = split_limbs(first * second)
    sums = [jnp.sum(limb.reshape(N_GX, CX, N_GY, CY, N_GZ, CZ), axis=(1, 3, 5), dtype=jnp.int32) for limb in limbs]
    blocks = normalize(sums)
    return combine(jnp.sum(blocks, axis=(0, 1, 2), dtype=jnp.int32))


def reference(right_side, cell_type, relax_weight):
    padded_type = jnp.pad(cell_type, 1)
    open_cells = (padded_type != 0).astype(jnp.float32)
    open_count = beside(open_cells)
    fluid_cell = (cell_type == 1).astype(jnp.float32)
    weight = fluid_cell * (relax_weight + open_count)

    def operate(field_in):
        return weight * field_in - fluid_cell * beside(jnp.pad(field_in, 1))

    pressure = jnp.zeros_like(right_side)
    residual = fluid_cell * right_side
    direction = residual
    norm_now = dot_field(residual, residual)
    for iteration in range(ITERS):
        image_field = operate(direction)
        step_size = norm_now / dot_field(direction, image_field)
        pressure = pressure + step_size * direction
        residual = residual - step_size * image_field
        norm_next = dot_field(residual, residual)
        direction = residual + (norm_next / norm_now) * direction
        norm_now = norm_next
    return pressure, residual
```

```python
import functools

import jax
import jax.numpy as jnp
from jax import lax
from jax.experimental import pallas as pl
from jax.experimental.pallas import tpu as pltpu
from jax.sharding import PartitionSpec as P

ITERS = 8
AXES = ("gx", "gy", "gz")
MESH = pl.DeviceIdType.MESH
LANES = 128
ROWS = 8
OPEN, START = 2, 3


def kernel(counts, rhs, kind, relax, pressure, residual, ext, hy, hz, sy, sz, p, s, z, n, weight, fluid,
           mine, others, hsend, hrecv, asend, arecv):
    cx, cy, cz = rhs.shape
    tiles = cy // ROWS
    me = tuple(lax.axis_index(a) for a in AXES)
    lane = lax.broadcasted_iota(jnp.int32, (ROWS, LANES), 1)
    row_of = lax.broadcasted_iota(jnp.int32, (cy, cz), 0)
    col_of = lax.broadcasted_iota(jnp.int32, (cy, cz), 1)

    offsets = [(a, b, c) for a in range(counts[0]) for b in range(counts[1]) for c in range(counts[2])][1:]
    offsets.sort(key=lambda o: -sum(min(v, m - v) for v, m in zip(o, counts)))
    my_row = (me[0] * counts[1] + me[1]) * counts[2] + me[2]

    def peer(o):
        return tuple(lax.rem(m + v, c) if v else m for m, v, c in zip(me, o, counts))

    barrier = pltpu.get_barrier_semaphore()

    def halo(b, axis, up):
        target = tuple(m + (1 if up else -1) if d == axis else m for d, m in enumerate(me))
        if axis == 0:
            src, dst = (ext.at[b, cx], ext.at[b, 0]) if up else (ext.at[b, 1], ext.at[b, cx + 1])
        elif axis == 1:
            src, dst = sy.at[b, 1 if up else 0], hy.at[b, 0 if up else 1]
        else:
            src, dst = sz.at[b, 1 if up else 0], hz.at[b, 0 if up else 1]
        where = 2 * axis + (0 if up else 1)
        return pltpu.make_async_remote_copy(
            src_ref=src, dst_ref=dst, send_sem=hsend.at[b, where], recv_sem=hrecv.at[b, where],
            device_id=target, device_id_type=MESH)

    def halo_do(b, axes, what):
        for axis in axes:
            if counts[axis] == 1:
                continue
            for up in (True, False):
                leaves = me[axis] < counts[axis] - 1 if up else me[axis] > 0
                reaches = me[axis] > 0 if up else me[axis] < counts[axis] - 1

                @pl.when(reaches if what == "recv" else leaves)
                def _():
                    copy = halo(b, axis, up)
                    if what == "start":
                        copy.start()
                    elif what == "recv":
                        copy.wait_recv()
                    else:
                        copy.wait_send()

    def pack_faces(b, x, value, packed):
        sy[b, 0, pl.ds(x, 1), :] = value[:1, :]
        sy[b, 1, pl.ds(x, 1), :] = value[cy - 1:, :]
        low, high = packed
        for t in range(tiles):
            q = t * cx + x
            rows = value[t * ROWS:(t + 1) * ROWS]
            low = jnp.where(lane == q, pltpu.roll(rows[:, :LANES], q, 1), low)
            high = jnp.where(lane == q, pltpu.roll(rows[:, cz - LANES:], lax.rem(q + 1, LANES), 1), high)
        return low, high

    def neighbours(b, x):
        centre = ext[b, x + 1]
        total = ext[b, x] + ext[b, x + 2]
        before = jnp.where(row_of == 0, hy[b, 0, pl.ds(x, 1), :], pltpu.roll(centre, 1, 0))
        after = jnp.where(row_of == cy - 1, hy[b, 1, pl.ds(x, 1), :], pltpu.roll(centre, cy - 1, 0))
        total = total + before + after
        first, last = hz[b, 0], hz[b, 1]
        lows = [pltpu.roll(first, lax.rem(LANES - (t * cx + x), LANES), 1) for t in range(tiles)]
        highs = [pltpu.roll(last, LANES - 1 - (t * cx + x), 1) for t in range(tiles)]
        reps = cz // LANES
        low = jnp.concatenate([jnp.concatenate(lows, 0)] * reps, 1)
        high = jnp.concatenate([jnp.concatenate(highs, 0)] * reps, 1)
        before = jnp.where(col_of == 0, low, pltpu.roll(centre, 1, 1))
        after = jnp.where(col_of == cz - 1, high, pltpu.roll(centre, cz - 1, 1))
        return centre, total + before + after

    def add_limbs(product, acc):
        whole = jnp.floor(product)
        frac = ((product - whole) * 16777216.0).astype(jnp.int32)
        whole = whole.astype(jnp.int32)

        def fold(v):
            parts = [v[i:i + ROWS, j:j + LANES] for i in range(0, v.shape[0], ROWS) for j in range(0, cz, LANES)]
            while len(parts) > 1:
                parts = [a + c for a, c in zip(parts[::2], parts[1::2])]
            return parts[0]

        frac, whole = fold(frac), fold(whole)
        a0, a1, a2, a3 = acc
        return (a0 + (frac & 4095), a1 + (frac >> 12), a2 + (whole & 4095), a3 + (whole >> 12))

    def ring_copy(k, i, o):
        return pltpu.make_async_remote_copy(
            src_ref=mine.at[k], dst_ref=others.at[k, pl.ds(my_row, 1)], send_sem=asend.at[k, i],
            recv_sem=arecv.at[k, i], device_id=peer(o), device_id_type=MESH)

    def send_sums(k, dots):
        rows = []
        for acc in dots:
            carry = None
            for level, v in enumerate(acc):
                v = v if carry is None else v + carry
                if level < 3:
                    carry = v >> 12
                    v = v & 4095
                rows.append(jnp.sum(v, axis=0, keepdims=True))
        block = jnp.concatenate(rows, 0)
        for shift in (64, 32, 16, 8, 4, 2, 1):
            block = block + pltpu.roll(block, shift, 1)
        diag = lane == lax.broadcasted_iota(jnp.int32, (ROWS, LANES), 0)
        mine[k] = jnp.sum(jnp.where(diag, block, 0), axis=0, keepdims=True)
        for i, o in enumerate(offsets):
            ring_copy(k, i, o).start()

    def wait_sums(k):
        for i, o in enumerate(offsets):
            ring_copy(k, i, o).wait_recv()
        total = jnp.sum(others[k], axis=0, keepdims=True) + mine[k]
        total = jnp.broadcast_to(total, (ROWS, LANES))
        level = lane & 3
        for _ in range(3):
            carry = jnp.where(level == 3, 0, total >> 12)
            total = jnp.where(level == 3, total, total & 4095) + pltpu.roll(carry, 1, 1)
        scale = jnp.where(level == 0, 1.0 / 16777216.0,
                          jnp.where(level == 1, 1.0 / 4096.0, jnp.where(level == 2, 1.0, 4096.0)))
        value = total.astype(jnp.float32) * scale
        value = value + pltpu.roll(value, LANES - 1, 1)
        value = value + pltpu.roll(value, LANES - 2, 1)
        return value[:1, 0:1], value[:1, 4:5]

    def done_sums(k):
        for i, o in enumerate(offsets):
            ring_copy(k, i, o).wait_send()

    def steps(gamma, delta, gamma_old, alpha_old):
        beta = gamma / gamma_old
        alpha = gamma / (delta - beta * gamma / alpha_old)
        return alpha, beta

    no_sums = tuple(jnp.zeros((ROWS, LANES), jnp.int32) for _ in range(4))
    no_faces = (jnp.zeros((ROWS, LANES), jnp.float32),) * 2

    edge = jnp.zeros((cy, cz), jnp.float32)
    for b in range(4):
        ext[b, 0] = edge
        ext[b, cx + 1] = edge
    hy[...] = jnp.zeros_like(hy)
    hz[...] = jnp.zeros_like(hz)
    others[...] = jnp.zeros_like(others)
    for o in offsets:
        pl.semaphore_signal(barrier, inc=1, device_id=peer(o), device_id_type=MESH)

    def first(x, carry):
        packed_open, packed_start = carry
        types = kind[x]
        is_fluid = jnp.where(types == 1, 1.0, 0.0)
        is_open = jnp.where(types != 0, 1.0, 0.0)
        start = is_fluid * rhs[x]
        fluid[x] = is_fluid
        ext[OPEN, x + 1] = is_open
        ext[START, x + 1] = start
        return pack_faces(OPEN, x, is_open, packed_open), pack_faces(START, x, start, packed_start)

    packed_open, packed_start = lax.fori_loop(0, cx, first, (no_faces, no_faces))
    for b, packed in ((OPEN, packed_open), (START, packed_start)):
        sz[b, 0], sz[b, 1] = packed
    pl.semaphore_wait(barrier, len(offsets))
    for b in (OPEN, START):
        halo_do(b, (0, 1, 2), "start")

    def clear(x, carry):
        for ref in (p, s, z, pressure):
            ref[x] = edge
        return carry

    lax.fori_loop(0, cx, clear, 0)
    for b in (OPEN, START):
        halo_do(b, (1, 2), "recv")

    def begin(x, carry):
        packed, norms, curves = carry
        _, count = neighbours(OPEN, x)
        weighed = fluid[x] * (relax[x] + count)
        weight[x] = weighed
        start, around = neighbours(START, x)
        image = weighed * start - fluid[x] * around
        ext[0, x + 1] = image
        return (pack_faces(0, x, image, packed), add_limbs(start * start, norms), add_limbs(start * image, curves))

    carry = lax.fori_loop(1, cx - 1, begin, (no_faces, no_sums, no_sums))
    for b in (OPEN, START):
        halo_do(b, (0,), "recv")
    carry = lax.fori_loop(0, 2, lambda i, c: begin(i * (cx - 1), c), carry)
    sz[0, 0], sz[0, 1] = carry[0]
    halo_do(0, (0, 1, 2), "start")
    send_sums(0, carry[1:])

    def apply(b):
        def one(x, carry):
            centre, around = neighbours(b, x)
            n[x] = weight[x] * centre - fluid[x] * around
            return carry

        halo_do(b, (1, 2), "recv")
        lax.fori_loop(1, cx - 1, one, 0)
        halo_do(b, (0,), "recv")
        lax.fori_loop(0, 2, lambda i, c: one(i * (cx - 1), c), 0)

    apply(0)
    for b in (OPEN, START):
        halo_do(b, (0, 1, 2), "send")

    def iteration(k, carry):
        b = lax.rem(k, 2)
        c = 1 - b
        gamma, delta = wait_sums(b)
        alpha, beta = steps(gamma, delta, *carry)
        halo_do(b, (0, 1, 2), "send")
        done_sums(b)

        def update(x, carry):
            packed, norms, curves = carry
            old = ext[b, x + 1]
            z_new = n[x] + beta * z[x]
            z[x] = z_new
            w_new = old - alpha * z_new
            ext[c, x + 1] = w_new
            s_new = old + beta * s[x]
            s[x] = s_new
            r_old = ext[START, x + 1]
            p_new = r_old + beta * p[x]
            p[x] = p_new
            pressure[x] = pressure[x] + alpha * p_new
            r_new = r_old - alpha * s_new
            ext[START, x + 1] = r_new
            return (pack_faces(c, x, w_new, packed), add_limbs(r_new * r_new, norms), add_limbs(r_new * w_new, curves))

        sums = lax.fori_loop(0, 2, lambda i, v: update(i * (cx - 1), v), (no_faces, no_sums, no_sums))
        @pl.when(k < ITERS - 2)
        def _():
            halo_do(c, (0,), "start")

        sums = lax.fori_loop(1, cx - 1, update, sums)
        sz[c, 0], sz[c, 1] = sums[0]

        @pl.when(k < ITERS - 2)
        def _():
            halo_do(c, (1, 2), "start")

        send_sums(c, sums[1:])

        @pl.when(k < ITERS - 2)
        def _():
            apply(c)

        return gamma, alpha

    carry = lax.fori_loop(0, ITERS - 1, iteration, (jnp.full((1, 1), jnp.inf, jnp.float32), jnp.ones((1, 1), jnp.float32)))
    b = (ITERS - 1) % 2
    gamma, delta = wait_sums(b)
    alpha, beta = steps(gamma, delta, *carry)
    done_sums(b)

    def finish(x, carry):
        s_new = ext[b, x + 1] + beta * s[x]
        r_old = ext[START, x + 1]
        pressure[x] = pressure[x] + alpha * (r_old + beta * p[x])
        residual[x] = r_old - alpha * s_new
        return carry

    lax.fori_loop(0, cx, finish, 0)


def solution(mesh):
    counts = tuple(mesh.shape[a] for a in AXES)
    total = counts[0] * counts[1] * counts[2]

    def on_device(right_side, cell_type, relax_weight):
        cx, cy, cz = right_side.shape
        field = pltpu.VMEM((cx, cy, cz), jnp.float32)
        out = jax.ShapeDtypeStruct(right_side.shape, jnp.float32)
        vmem = pl.BlockSpec(memory_space=pltpu.VMEM)
        return pl.pallas_call(
            functools.partial(kernel, counts),
            out_shape=(out, out),
            in_specs=[vmem] * 3,
            out_specs=(vmem, vmem),
            scratch_shapes=[
                pltpu.VMEM((4, cx + 2, cy, cz), jnp.float32),
                pltpu.VMEM((4, 2, cx, cz), jnp.float32),
                pltpu.VMEM((4, 2, ROWS, LANES), jnp.float32),
                pltpu.VMEM((4, 2, cx, cz), jnp.float32),
                pltpu.VMEM((4, 2, ROWS, LANES), jnp.float32),
                field, field, field, field, field, field,
                pltpu.VMEM((2, 1, LANES), jnp.int32),
                pltpu.VMEM((2, total, LANES), jnp.int32),
                pltpu.SemaphoreType.DMA((4, 6)),
                pltpu.SemaphoreType.DMA((4, 6)),
                pltpu.SemaphoreType.DMA((2, total - 1)),
                pltpu.SemaphoreType.DMA((2, total - 1)),
            ],
            compiler_params=pltpu.CompilerParams(collective_id=0, has_side_effects=True),
        )(right_side, cell_type, relax_weight)

    spec = P(*AXES)
    return jax.shard_map(
        on_device, mesh=mesh, in_specs=(spec, spec, spec), out_specs=(spec, spec), check_vma=False)
```

```python
import functools

import jax
import jax.numpy as jnp
from jax import lax
from jax.experimental import pallas as pl
from jax.experimental.pallas import tpu as pltpu
from jax.sharding import PartitionSpec as P

ITERS = 8
AXES = ("gx", "gy", "gz")
MESH = pl.DeviceIdType.MESH
LANES = 128
ROWS = 8
OPEN, START = 2, 3


def kernel(counts, rhs_in, kind_in, relax_in, pressure_out, residual_out, rhs, kind, relax, pressure, residual, io, ext, hy, hz, sy, sz, p, s, z, n, weight, fluid,
           mine, others, hsend, hrecv, asend, arecv):
    cx, cy, cz = rhs.shape
    tiles = cy // ROWS
    me = tuple(lax.axis_index(a) for a in AXES)
    lane = lax.broadcasted_iota(jnp.int32, (ROWS, LANES), 1)
    row_of = lax.broadcasted_iota(jnp.int32, (cy, cz), 0)
    col_of = lax.broadcasted_iota(jnp.int32, (cy, cz), 1)

    offsets = [(a, b, c) for a in range(counts[0]) for b in range(counts[1]) for c in range(counts[2])][1:]
    offsets.sort(key=lambda o: -sum(min(v, m - v) for v, m in zip(o, counts)))
    my_row = (me[0] * counts[1] + me[1]) * counts[2] + me[2]

    def peer(o):
        return tuple(lax.rem(m + v, c) if v else m for m, v, c in zip(me, o, counts))

    loads = [pltpu.make_async_copy(src, dst, io.at[i])
             for i, (src, dst) in enumerate(((kind_in, kind), (rhs_in, rhs), (relax_in, relax)))]
    for load in loads:
        load.start()
    barrier = pltpu.get_barrier_semaphore()

    def halo(b, axis, up):
        target = tuple(m + (1 if up else -1) if d == axis else m for d, m in enumerate(me))
        if axis == 0:
            src, dst = (ext.at[b, cx], ext.at[b, 0]) if up else (ext.at[b, 1], ext.at[b, cx + 1])
        elif axis == 1:
            src, dst = sy.at[b, 1 if up else 0], hy.at[b, 0 if up else 1]
        else:
            src, dst = sz.at[b, 1 if up else 0], hz.at[b, 0 if up else 1]
        where = 2 * axis + (0 if up else 1)
        return pltpu.make_async_remote_copy(
            src_ref=src, dst_ref=dst, send_sem=hsend.at[b, where], recv_sem=hrecv.at[b, where],
            device_id=target, device_id_type=MESH)

    def halo_do(b, axes, what):
        for axis in axes:
            if counts[axis] == 1:
                continue
            for up in (True, False):
                leaves = me[axis] < counts[axis] - 1 if up else me[axis] > 0
                reaches = me[axis] > 0 if up else me[axis] < counts[axis] - 1

                @pl.when(reaches if what == "recv" else leaves)
                def _():
                    copy = halo(b, axis, up)
                    if what == "start":
                        copy.start()
                    elif what == "recv":
                        copy.wait_recv()
                    else:
                        copy.wait_send()

    def pack_faces(b, x, value, packed):
        sy[b, 0, pl.ds(x, 1), :] = value[:1, :]
        sy[b, 1, pl.ds(x, 1), :] = value[cy - 1:, :]
        low, high = packed
        for t in range(tiles):
            q = t * cx + x
            rows = value[t * ROWS:(t + 1) * ROWS]
            low = jnp.where(lane == q, pltpu.roll(rows[:, :LANES], q, 1), low)
            high = jnp.where(lane == q, pltpu.roll(rows[:, cz - LANES:], lax.rem(q + 1, LANES), 1), high)
        return low, high

    def neighbours(b, x):
        centre = ext[b, x + 1]
        total = ext[b, x] + ext[b, x + 2]
        before = jnp.where(row_of == 0, hy[b, 0, pl.ds(x, 1), :], pltpu.roll(centre, 1, 0))
        after = jnp.where(row_of == cy - 1, hy[b, 1, pl.ds(x, 1), :], pltpu.roll(centre, cy - 1, 0))
        total = total + before + after
        first, last = hz[b, 0], hz[b, 1]
        lows = [pltpu.roll(first, lax.rem(LANES - (t * cx + x), LANES), 1) for t in range(tiles)]
        highs = [pltpu.roll(last, LANES - 1 - (t * cx + x), 1) for t in range(tiles)]
        reps = cz // LANES
        low = jnp.concatenate([jnp.concatenate(lows, 0)] * reps, 1)
        high = jnp.concatenate([jnp.concatenate(highs, 0)] * reps, 1)
        before = jnp.where(col_of == 0, low, pltpu.roll(centre, 1, 1))
        after = jnp.where(col_of == cz - 1, high, pltpu.roll(centre, cz - 1, 1))
        return centre, total + before + after

    def add_limbs(product, acc):
        whole = jnp.floor(product)
        frac = ((product - whole) * 16777216.0).astype(jnp.int32)
        whole = whole.astype(jnp.int32)

        def fold(v):
            parts = [v[i:i + ROWS, j:j + LANES] for i in range(0, v.shape[0], ROWS) for j in range(0, cz, LANES)]
            while len(parts) > 1:
                parts = [a + c for a, c in zip(parts[::2], parts[1::2])]
            return parts[0]

        frac, whole = fold(frac), fold(whole)
        a0, a1, a2, a3 = acc
        return (a0 + (frac & 4095), a1 + (frac >> 12), a2 + (whole & 4095), a3 + (whole >> 12))

    def ring_copy(k, i, o):
        return pltpu.make_async_remote_copy(
            src_ref=mine.at[k], dst_ref=others.at[k, pl.ds(my_row, 1)], send_sem=asend.at[k, i],
            recv_sem=arecv.at[k, i], device_id=peer(o), device_id_type=MESH)

    def send_sums(k, dots):
        rows = []
        for acc in dots:
            carry = None
            for level, v in enumerate(acc):
                v = v if carry is None else v + carry
                if level < 3:
                    carry = v >> 12
                    v = v & 4095
                rows.append(jnp.sum(v, axis=0, keepdims=True))
        block = jnp.concatenate(rows, 0)
        block = jnp.sum(block, axis=1, keepdims=True)
        diag = lane == lax.broadcasted_iota(jnp.int32, (ROWS, LANES), 0)
        mine[k] = jnp.sum(jnp.where(diag, block, 0), axis=0, keepdims=True)
        for i, o in enumerate(offsets):
            ring_copy(k, i, o).start()

    def wait_sums(k):
        for i, o in enumerate(offsets):
            ring_copy(k, i, o).wait_recv()
        total = jnp.sum(others[k], axis=0, keepdims=True) + mine[k]
        total = jnp.broadcast_to(total, (ROWS, LANES))
        level = lane & 3
        for _ in range(3):
            carry = jnp.where(level == 3, 0, total >> 12)
            total = jnp.where(level == 3, total, total & 4095) + pltpu.roll(carry, 1, 1)
        scale = jnp.where(level == 0, 1.0 / 16777216.0,
                          jnp.where(level == 1, 1.0 / 4096.0, jnp.where(level == 2, 1.0, 4096.0)))
        value = total.astype(jnp.float32) * scale
        value = value + pltpu.roll(value, LANES - 1, 1)
        value = value + pltpu.roll(value, LANES - 2, 1)
        return value[:1, 0:1], value[:1, 4:5]

    def done_sums(k):
        for i, o in enumerate(offsets):
            ring_copy(k, i, o).wait_send()

    def steps(gamma, delta, gamma_old, alpha_old):
        beta = gamma / gamma_old
        alpha = gamma / (delta - beta * gamma / alpha_old)
        return alpha, beta

    no_sums = tuple(jnp.zeros((ROWS, LANES), jnp.int32) for _ in range(4))
    no_faces = (jnp.zeros((ROWS, LANES), jnp.float32),) * 2

    edge = jnp.zeros((cy, cz), jnp.float32)
    for b in range(4):
        ext[b, 0] = edge
        ext[b, cx + 1] = edge
    hy[...] = jnp.zeros_like(hy)
    hz[...] = jnp.zeros_like(hz)
    others[...] = jnp.zeros_like(others)
    for o in offsets:
        pl.semaphore_signal(barrier, inc=1, device_id=peer(o), device_id_type=MESH)

    def first(x, carry):
        packed_open, packed_start = carry
        types = kind[x]
        is_fluid = jnp.where(types == 1, 1.0, 0.0)
        is_open = jnp.where(types != 0, 1.0, 0.0)
        start = is_fluid * rhs[x]
        fluid[x] = is_fluid
        ext[OPEN, x + 1] = is_open
        ext[START, x + 1] = start
        return pack_faces(OPEN, x, is_open, packed_open), pack_faces(START, x, start, packed_start)

    for load in loads:
        load.wait()
    packed_open, packed_start = lax.fori_loop(0, cx, first, (no_faces, no_faces))
    for b, packed in ((OPEN, packed_open), (START, packed_start)):
        sz[b, 0], sz[b, 1] = packed
    pl.semaphore_wait(barrier, len(offsets))
    for b in (OPEN, START):
        halo_do(b, (0, 1, 2), "start")

    def clear(x, carry):
        for ref in (p, s, z, pressure):
            ref[x] = edge
        return carry

    lax.fori_loop(0, cx, clear, 0)
    for b in (OPEN, START):
        halo_do(b, (1, 2), "recv")

    def begin(x, carry):
        packed, norms, curves = carry
        _, count = neighbours(OPEN, x)
        weighed = fluid[x] * (relax[x] + count)
        weight[x] = weighed
        start, around = neighbours(START, x)
        image = weighed * start - fluid[x] * around
        ext[0, x + 1] = image
        return (pack_faces(0, x, image, packed), add_limbs(start * start, norms), add_limbs(start * image, curves))

    carry = lax.fori_loop(1, cx - 1, begin, (no_faces, no_sums, no_sums))
    for b in (OPEN, START):
        halo_do(b, (0,), "recv")
    carry = lax.fori_loop(0, 2, lambda i, c: begin(i * (cx - 1), c), carry)
    sz[0, 0], sz[0, 1] = carry[0]
    halo_do(0, (0, 1, 2), "start")
    send_sums(0, carry[1:])

    def apply(b):
        def one(x, carry):
            centre, around = neighbours(b, x)
            n[x] = weight[x] * centre - fluid[x] * around
            return carry

        def pair(i, carry):
            return one(2 * i + 2, one(2 * i + 1, carry))

        halo_do(b, (1, 2), "recv")
        lax.fori_loop(0, (cx - 2) // 2, pair, 0)
        if cx % 2:
            one(cx - 2, 0)
        halo_do(b, (0,), "recv")
        one(cx - 1, one(0, 0))

    apply(0)
    for b in (OPEN, START):
        halo_do(b, (0, 1, 2), "send")

    def iteration(k, carry):
        b = lax.rem(k, 2)
        c = 1 - b
        gamma, delta = wait_sums(b)
        alpha, beta = steps(gamma, delta, *carry)
        halo_do(b, (0, 1, 2), "send")
        done_sums(b)

        def update(x, carry):
            packed, norms, curves = carry
            z_new = n[x] + beta * z[x]
            z[x] = z_new
            w_old = ext[b, x + 1]
            s_new = w_old + beta * s[x]
            s[x] = s_new
            w_new = w_old - alpha * z_new
            ext[c, x + 1] = w_new
            r_old = ext[START + b, x + 1]
            r_new = r_old - alpha * s_new
            ext[START + c, x + 1] = r_new
            return (pack_faces(c, x, w_new, packed), add_limbs(r_new * r_new, norms), add_limbs(r_new * w_new, curves))

        sums = lax.fori_loop(0, 2, lambda i, v: update(i * (cx - 1), v), (no_faces, no_sums, no_sums))

        @pl.when(k < ITERS - 2)
        def _():
            halo_do(c, (0,), "start")

        sums = lax.fori_loop(1, cx - 1, update, sums)
        sz[c, 0], sz[c, 1] = sums[0]

        @pl.when(k < ITERS - 2)
        def _():
            halo_do(c, (1, 2), "start")

        send_sums(c, sums[1:])

        def follow(x, carry):
            p_new = ext[START + b, x + 1] + beta * p[x]
            p[x] = p_new
            pressure[x] = pressure[x] + alpha * p_new
            return carry

        lax.fori_loop(0, cx, follow, 0)

        @pl.when(k < ITERS - 2)
        def _():
            apply(c)

        return gamma, alpha

    carry = lax.fori_loop(0, ITERS - 1, iteration, (jnp.full((1, 1), jnp.inf, jnp.float32), jnp.ones((1, 1), jnp.float32)))
    b = (ITERS - 1) % 2
    gamma, delta = wait_sums(b)
    alpha, beta = steps(gamma, delta, *carry)
    done_sums(b)

    def finish(x, carry):
        s_new = ext[b, x + 1] + beta * s[x]
        r_old = ext[START + b, x + 1]
        pressure[x] = pressure[x] + alpha * (r_old + beta * p[x])
        residual[x] = r_old - alpha * s_new
        return carry

    stores = []
    parts = next(m for m in (4, 2, 1) if cx % m == 0)
    for i in range(parts):
        size = cx // parts
        lax.fori_loop(i * size, (i + 1) * size, finish, 0)
        for j, (src, dst) in enumerate(((pressure, pressure_out), (residual, residual_out))):
            where = pl.ds(i * size, size)
            stores.append(pltpu.make_async_copy(src.at[where], dst.at[where], io.at[3 + 2 * i + j]))
            stores[-1].start()
    for store in stores:
        store.wait()


def solution(mesh):
    counts = tuple(mesh.shape[a] for a in AXES)
    total = counts[0] * counts[1] * counts[2]

    def on_device(right_side, cell_type, relax_weight):
        cx, cy, cz = right_side.shape
        field = pltpu.VMEM((cx, cy, cz), jnp.float32)
        out = jax.ShapeDtypeStruct(right_side.shape, jnp.float32)
        whole = pl.BlockSpec(memory_space=pl.ANY)
        return pl.pallas_call(
            functools.partial(kernel, counts),
            out_shape=(out, out),
            in_specs=[whole] * 3,
            out_specs=(whole, whole),
            scratch_shapes=[
                field, pltpu.VMEM((cx, cy, cz), jnp.int32), field, field, field,
                pltpu.SemaphoreType.DMA((11,)),
                pltpu.VMEM((5, cx + 2, cy, cz), jnp.float32),
                pltpu.VMEM((4, 2, cx, cz), jnp.float32),
                pltpu.VMEM((4, 2, ROWS, LANES), jnp.float32),
                pltpu.VMEM((4, 2, cx, cz), jnp.float32),
                pltpu.VMEM((4, 2, ROWS, LANES), jnp.float32),
                field, field, field, field, field, field,
                pltpu.VMEM((2, 1, LANES), jnp.int32),
                pltpu.VMEM((2, total, LANES), jnp.int32),
                pltpu.SemaphoreType.DMA((4, 6)),
                pltpu.SemaphoreType.DMA((4, 6)),
                pltpu.SemaphoreType.DMA((2, total - 1)),
                pltpu.SemaphoreType.DMA((2, total - 1)),
            ],
            compiler_params=pltpu.CompilerParams(collective_id=0, has_side_effects=True),
        )(right_side, cell_type, relax_weight)

    spec = P(*AXES)
    return jax.shard_map(
        on_device, mesh=mesh, in_specs=(spec, spec, spec), out_specs=(spec, spec), check_vma=False)
```

```python
import functools

import jax
import jax.numpy as jnp
from jax import lax
from jax.experimental import pallas as pl
from jax.experimental.pallas import tpu as pltpu
from jax.sharding import PartitionSpec as P

ITERS = 8
AXES = ("gx", "gy", "gz")
MESH = pl.DeviceIdType.MESH
LANES = 128
ROWS = 8
OPEN, START = 2, 3


def kernel(counts, rhs_in, kind_in, relax_in, pressure_out, residual_out, rhs, kind, relax, pressure, residual, io, ext, hy, hz, sy, sz, p, s, z, n, weight, fluid,
           mine, others, hsend, hrecv, asend, arecv):
    cx, cy, cz = rhs.shape
    tiles = cy // ROWS
    me = tuple(lax.axis_index(a) for a in AXES)
    lane = lax.broadcasted_iota(jnp.int32, (ROWS, LANES), 1)
    row_of = lax.broadcasted_iota(jnp.int32, (cy, cz), 0)
    col_of = lax.broadcasted_iota(jnp.int32, (cy, cz), 1)

    offsets = [(a, b, c) for a in range(counts[0]) for b in range(counts[1]) for c in range(counts[2])][1:]
    offsets.sort(key=lambda o: -sum(min(v, m - v) for v, m in zip(o, counts)))
    my_row = (me[0] * counts[1] + me[1]) * counts[2] + me[2]

    def peer(o):
        return tuple(lax.rem(m + v, c) if v else m for m, v, c in zip(me, o, counts))

    loads = [pltpu.make_async_copy(src, dst, io.at[i])
             for i, (src, dst) in enumerate(((kind_in, kind), (rhs_in, rhs), (relax_in, relax)))]
    for load in loads:
        load.start()
    barrier = pltpu.get_barrier_semaphore()

    def halo(b, axis, up):
        target = tuple(m + (1 if up else -1) if d == axis else m for d, m in enumerate(me))
        if axis == 0:
            src, dst = (ext.at[b, cx], ext.at[b, 0]) if up else (ext.at[b, 1], ext.at[b, cx + 1])
        elif axis == 1:
            src, dst = sy.at[b, 1 if up else 0], hy.at[b, 0 if up else 1]
        else:
            src, dst = sz.at[b, 1 if up else 0], hz.at[b, 0 if up else 1]
        where = 2 * axis + (0 if up else 1)
        return pltpu.make_async_remote_copy(
            src_ref=src, dst_ref=dst, send_sem=hsend.at[b, where], recv_sem=hrecv.at[b, where],
            device_id=target, device_id_type=MESH)

    def halo_do(b, axes, what):
        for axis in axes:
            if counts[axis] == 1:
                continue
            for up in (True, False):
                leaves = me[axis] < counts[axis] - 1 if up else me[axis] > 0
                reaches = me[axis] > 0 if up else me[axis] < counts[axis] - 1

                @pl.when(reaches if what == "recv" else leaves)
                def _():
                    copy = halo(b, axis, up)
                    if what == "start":
                        copy.start()
                    elif what == "recv":
                        copy.wait_recv()
                    else:
                        copy.wait_send()

    def pack_faces(b, x, value, packed):
        sy[b, 0, pl.ds(x, 1), :] = value[:1, :]
        sy[b, 1, pl.ds(x, 1), :] = value[cy - 1:, :]
        low, high = packed
        for t in range(tiles):
            q = t * cx + x
            rows = value[t * ROWS:(t + 1) * ROWS]
            low = jnp.where(lane == q, pltpu.roll(rows[:, :LANES], q, 1), low)
            high = jnp.where(lane == q, pltpu.roll(rows[:, cz - LANES:], lax.rem(q + 1, LANES), 1), high)
        return low, high

    def neighbours(b, x):
        centre = ext[b, x + 1]
        total = ext[b, x] + ext[b, x + 2]
        before = jnp.where(row_of == 0, hy[b, 0, pl.ds(x, 1), :], pltpu.roll(centre, 1, 0))
        after = jnp.where(row_of == cy - 1, hy[b, 1, pl.ds(x, 1), :], pltpu.roll(centre, cy - 1, 0))
        total = total + before + after
        first, last = hz[b, 0], hz[b, 1]
        lows = [pltpu.roll(first, lax.rem(LANES - (t * cx + x), LANES), 1) for t in range(tiles)]
        highs = [pltpu.roll(last, LANES - 1 - (t * cx + x), 1) for t in range(tiles)]
        reps = cz // LANES
        low = jnp.concatenate([jnp.concatenate(lows, 0)] * reps, 1)
        high = jnp.concatenate([jnp.concatenate(highs, 0)] * reps, 1)
        before = jnp.where(col_of == 0, low, pltpu.roll(centre, 1, 1))
        after = jnp.where(col_of == cz - 1, high, pltpu.roll(centre, cz - 1, 1))
        return centre, total + before + after

    def add_limbs(product, acc):
        whole = jnp.floor(product)
        frac = ((product - whole) * 16777216.0).astype(jnp.int32)
        whole = whole.astype(jnp.int32)

        def fold(v):
            parts = [v[i:i + ROWS, j:j + LANES] for i in range(0, v.shape[0], ROWS) for j in range(0, cz, LANES)]
            while len(parts) > 1:
                parts = [a + c for a, c in zip(parts[::2], parts[1::2])]
            return parts[0]

        frac, whole = fold(frac), fold(whole)
        a0, a1, a2, a3 = acc
        return (a0 + (frac & 4095), a1 + (frac >> 12), a2 + (whole & 4095), a3 + (whole >> 12))

    def ring_copy(k, i, o):
        return pltpu.make_async_remote_copy(
            src_ref=mine.at[k], dst_ref=others.at[k, pl.ds(my_row, 1)], send_sem=asend.at[k, i],
            recv_sem=arecv.at[k, i], device_id=peer(o), device_id_type=MESH)

    def send_sums(k, dots):
        rows = []
        for acc in dots:
            carry = None
            for level, v in enumerate(acc):
                v = v if carry is None else v + carry
                if level < 3:
                    carry = v >> 12
                    v = v & 4095
                rows.append(jnp.sum(v, axis=0, keepdims=True))
        block = jnp.concatenate(rows, 0)
        block = jnp.sum(block, axis=1, keepdims=True)
        diag = lane == lax.broadcasted_iota(jnp.int32, (ROWS, LANES), 0)
        mine[k] = jnp.sum(jnp.where(diag, block, 0), axis=0, keepdims=True)
        for i, o in enumerate(offsets):
            ring_copy(k, i, o).start()

    def wait_sums(k):
        for i, o in enumerate(offsets):
            ring_copy(k, i, o).wait_recv()
        total = jnp.sum(others[k], axis=0, keepdims=True) + mine[k]
        total = jnp.broadcast_to(total, (ROWS, LANES))
        level = lane & 3
        for _ in range(3):
            carry = jnp.where(level == 3, 0, total >> 12)
            total = jnp.where(level == 3, total, total & 4095) + pltpu.roll(carry, 1, 1)
        scale = jnp.where(level == 0, 1.0 / 16777216.0,
                          jnp.where(level == 1, 1.0 / 4096.0, jnp.where(level == 2, 1.0, 4096.0)))
        value = total.astype(jnp.float32) * scale
        value = value + pltpu.roll(value, LANES - 1, 1)
        value = value + pltpu.roll(value, LANES - 2, 1)
        return value[:1, 0:1], value[:1, 4:5]

    def done_sums(k):
        for i, o in enumerate(offsets):
            ring_copy(k, i, o).wait_send()

    def steps(gamma, delta, gamma_old, alpha_old):
        beta = gamma / gamma_old
        alpha = gamma / (delta - beta * gamma / alpha_old)
        return alpha, beta

    no_sums = tuple(jnp.zeros((ROWS, LANES), jnp.int32) for _ in range(4))
    no_faces = (jnp.zeros((ROWS, LANES), jnp.float32),) * 2

    edge = jnp.zeros((cy, cz), jnp.float32)
    for b in range(4):
        ext[b, 0] = edge
        ext[b, cx + 1] = edge
    hy[...] = jnp.zeros_like(hy)
    hz[...] = jnp.zeros_like(hz)
    others[...] = jnp.zeros_like(others)
    for o in offsets:
        pl.semaphore_signal(barrier, inc=1, device_id=peer(o), device_id_type=MESH)

    def first(x, carry):
        packed_open, packed_start = carry
        types = kind[x]
        is_fluid = jnp.where(types == 1, 1.0, 0.0)
        is_open = jnp.where(types != 0, 1.0, 0.0)
        start = is_fluid * rhs[x]
        fluid[x] = is_fluid
        ext[OPEN, x + 1] = is_open
        ext[START, x + 1] = start
        return pack_faces(OPEN, x, is_open, packed_open), pack_faces(START, x, start, packed_start)

    for load in loads:
        load.wait()
    packed_open, packed_start = lax.fori_loop(0, cx, first, (no_faces, no_faces))
    for b, packed in ((OPEN, packed_open), (START, packed_start)):
        sz[b, 0], sz[b, 1] = packed
    pl.semaphore_wait(barrier, len(offsets))
    for b in (OPEN, START):
        halo_do(b, (0, 1, 2), "start")

    def clear(x, carry):
        for ref in (p, s, z, pressure):
            ref[x] = edge
        return carry

    lax.fori_loop(0, cx, clear, 0)
    for b in (OPEN, START):
        halo_do(b, (1, 2), "recv")

    def begin(x, carry):
        packed, norms, curves = carry
        _, count = neighbours(OPEN, x)
        weighed = fluid[x] * (relax[x] + count)
        weight[x] = weighed
        start, around = neighbours(START, x)
        image = weighed * start - fluid[x] * around
        ext[0, x + 1] = image
        return (pack_faces(0, x, image, packed), add_limbs(start * start, norms), add_limbs(start * image, curves))

    carry = lax.fori_loop(1, cx - 1, begin, (no_faces, no_sums, no_sums))
    for b in (OPEN, START):
        halo_do(b, (0,), "recv")
    carry = lax.fori_loop(0, 2, lambda i, c: begin(i * (cx - 1), c), carry)
    sz[0, 0], sz[0, 1] = carry[0]
    halo_do(0, (0, 1, 2), "start")
    send_sums(0, carry[1:])

    def apply(b):
        def one(x, carry):
            centre, around = neighbours(b, x)
            n[x] = weight[x] * centre - fluid[x] * around
            return carry

        def pair(i, carry):
            return one(2 * i + 2, one(2 * i + 1, carry))

        halo_do(b, (1, 2), "recv")
        lax.fori_loop(0, (cx - 2) // 2, pair, 0)
        if cx % 2:
            one(cx - 2, 0)
        halo_do(b, (0,), "recv")
        one(cx - 1, one(0, 0))

    apply(0)
    for b in (OPEN, START):
        halo_do(b, (0, 1, 2), "send")

    def iteration(k, carry):
        b = lax.rem(k, 2)
        c = 1 - b
        gamma, delta = wait_sums(b)
        alpha, beta = steps(gamma, delta, *carry)
        halo_do(b, (0, 1, 2), "send")
        done_sums(b)

        def update(x, carry):
            packed, norms, curves = carry
            z_new = n[x] + beta * z[x]
            z[x] = z_new
            w_old = ext[b, x + 1]
            s_new = w_old + beta * s[x]
            s[x] = s_new
            w_new = w_old - alpha * z_new
            ext[c, x + 1] = w_new
            r_old = ext[START + b, x + 1]
            r_new = r_old - alpha * s_new
            ext[START + c, x + 1] = r_new
            return (pack_faces(c, x, w_new, packed), add_limbs(r_new * r_new, norms), add_limbs(r_new * w_new, curves))

        sums = lax.fori_loop(0, 2, lambda i, v: update(i * (cx - 1), v), (no_faces, no_sums, no_sums))

        @pl.when(k < ITERS - 2)
        def _():
            halo_do(c, (0,), "start")

        sums = lax.fori_loop(1, cx - 1, update, sums)
        sz[c, 0], sz[c, 1] = sums[0]

        send_sums(c, sums[1:])

        @pl.when(k < ITERS - 2)
        def _():
            halo_do(c, (1, 2), "start")

        def follow(x, carry):
            p_new = ext[START + b, x + 1] + beta * p[x]
            p[x] = p_new
            pressure[x] = pressure[x] + alpha * p_new
            return carry

        lax.fori_loop(0, cx, follow, 0)

        @pl.when(k < ITERS - 2)
        def _():
            apply(c)

        return gamma, alpha

    carry = lax.fori_loop(0, ITERS - 1, iteration, (jnp.full((1, 1), jnp.inf, jnp.float32), jnp.ones((1, 1), jnp.float32)))
    b = (ITERS - 1) % 2
    gamma, delta = wait_sums(b)
    alpha, beta = steps(gamma, delta, *carry)
    done_sums(b)

    def finish(x, carry):
        s_new = ext[b, x + 1] + beta * s[x]
        r_old = ext[START + b, x + 1]
        pressure[x] = pressure[x] + alpha * (r_old + beta * p[x])
        residual[x] = r_old - alpha * s_new
        return carry

    stores = []
    parts = next(m for m in (4, 2, 1) if cx % m == 0)
    for i in range(parts):
        size = cx // parts
        lax.fori_loop(i * size, (i + 1) * size, finish, 0)
        for j, (src, dst) in enumerate(((pressure, pressure_out), (residual, residual_out))):
            where = pl.ds(i * size, size)
            stores.append(pltpu.make_async_copy(src.at[where], dst.at[where], io.at[3 + 2 * i + j]))
            stores[-1].start()
    for store in stores:
        store.wait()


def solution(mesh):
    counts = tuple(mesh.shape[a] for a in AXES)
    total = counts[0] * counts[1] * counts[2]

    def on_device(right_side, cell_type, relax_weight):
        cx, cy, cz = right_side.shape
        field = pltpu.VMEM((cx, cy, cz), jnp.float32)
        out = jax.ShapeDtypeStruct(right_side.shape, jnp.float32)
        whole = pl.BlockSpec(memory_space=pl.ANY)
        return pl.pallas_call(
            functools.partial(kernel, counts),
            out_shape=(out, out),
            in_specs=[whole] * 3,
            out_specs=(whole, whole),
            scratch_shapes=[
                field, pltpu.VMEM((cx, cy, cz), jnp.int32), field, field, field,
                pltpu.SemaphoreType.DMA((11,)),
                pltpu.VMEM((5, cx + 2, cy, cz), jnp.float32),
                pltpu.VMEM((4, 2, cx, cz), jnp.float32),
                pltpu.VMEM((4, 2, ROWS, LANES), jnp.float32),
                pltpu.VMEM((4, 2, cx, cz), jnp.float32),
                pltpu.VMEM((4, 2, ROWS, LANES), jnp.float32),
                field, field, field, field, field, field,
                pltpu.VMEM((2, 1, LANES), jnp.int32),
                pltpu.VMEM((2, total, LANES), jnp.int32),
                pltpu.SemaphoreType.DMA((4, 6)),
                pltpu.SemaphoreType.DMA((4, 6)),
                pltpu.SemaphoreType.DMA((2, total - 1)),
                pltpu.SemaphoreType.DMA((2, total - 1)),
            ],
            compiler_params=pltpu.CompilerParams(collective_id=0, has_side_effects=True),
        )(right_side, cell_type, relax_weight)

    spec = P(*AXES)
    return jax.shard_map(
        on_device, mesh=mesh, in_specs=(spec, spec, spec), out_specs=(spec, spec), check_vma=False)
```
